8 devices in a mesh: dp: 1 (over z), tp: 2 (over y), ep: 4 (over x, core).
Axes of the slice: x: 2, y: 2, z: 1, core: 2. Of those that a mesh axis runs over, the one named last changes fastest.
Arguments:
- hidden: bfloat16 [256, 2048], P(('dp', 'ep'))
- expert_ids: int32 [256, 8], P(('dp', 'ep'))
- norm_w: bfloat16 [2048], replicated
- router_w: bfloat16 [2048, 64], replicated
- w_gate: bfloat16 [64, 2048, 1024], P('ep', None, 'tp')
- w_up: bfloat16 [64, 2048, 1024], P('ep', None, 'tp')
- w_down: bfloat16 [64, 1024, 2048], P('ep', 'tp')
Outputs:
- output: bfloat16 [256, 2048], P(('dp', 'ep'))
All inputs are finite; a program needn't handle non-finite values.
Results may differ from the reference program's by a relative error of at most 0.00947046.
Values are sent between devices in bfloat16 or wider.
A program may use at most 1 GiB of HBM per device.

```python
import jax
import jax.numpy as jnp
from jax import lax

D = 2048
FF = 1024
EXPERTS = 64
TOP = 8
TOK_DEV = 64
EP = 4
CAP = 16
TOKENS = TOK_DEV * EP
NORM_EPS = 1e-6


def random_order(order_key, count):
    order_score = jax.random.randint(order_key, (count,), 0, count) * count + jnp.arange(count, dtype=jnp.int32)
    return jnp.argsort(order_score)


def draw_routes(route_key):
    pair_count = TOP * TOK_DEV
    weight_total = (EXPERTS - 1) * (5 * EXPERTS - 2) // 2
    bounds = [CAP + ((pair_count - CAP) * (4 * rank_step * (EXPERTS - 1) - 3 * rank_step * (rank_step - 1) // 2)) // weight_total for rank_step in range(EXPERTS - 1)]
    bound_arr = jnp.array(bounds, dtype=jnp.int32)
    positions = jnp.arange(TOK_DEV, dtype=jnp.int32)[:, None] + TOK_DEV * jnp.arange(TOP, dtype=jnp.int32)[None, :]
    rank_of = jnp.sum((positions[:, :, None] >= bound_arr).astype(jnp.int32), axis=-1)
    label_key, rows_key = jax.random.split(route_key)
    labels = random_order(label_key, EXPERTS).astype(jnp.int32)
    choices = labels[rank_of]
    row_keys = jax.random.split(rows_key, EP)
    orders = jax.vmap(lambda sub_key: random_order(sub_key, TOK_DEV))(row_keys)
    return choices[orders].reshape(TOKENS, TOP).astype(jnp.int32)


def setup_inputs(seed: int = 0, part: int = 0) -> dict:
    base_key = jax.random.key(seed)
    key_list = jax.random.split(base_key, 7)
    hidden = jax.random.normal(jax.random.fold_in(key_list[0], part), (TOKENS, D), jnp.float32)
    expert_ids = draw_routes(jax.random.fold_in(key_list[1], part))
    norm_w = 1.0 + 0.3 * jax.random.normal(key_list[2], (D,), jnp.float32)
    router_w = D ** -0.5 * jax.random.normal(key_list[3], (D, EXPERTS), jnp.float32)
    w_gate = D ** -0.5 * jax.random.normal(key_list[4], (EXPERTS, D, FF), jnp.float32)
    w_up = D ** -0.5 * jax.random.normal(key_list[5], (EXPERTS, D, FF), jnp.float32)
    down_scale = 2.0 * EXPERTS / (TOP * FF) ** 0.5
    w_down = down_scale * jax.random.normal(key_list[6], (EXPERTS, FF, D), jnp.float32)
    return {"hidden": hidden.astype(jnp.bfloat16), "expert_ids": expert_ids, "norm_w": norm_w.astype(jnp.bfloat16), "router_w": router_w.astype(jnp.bfloat16), "w_gate": w_gate.astype(jnp.bfloat16), "w_up": w_up.astype(jnp.bfloat16), "w_down": w_down.astype(jnp.bfloat16)}


def rms_norm(hidden, norm_w):
    wide_h = hidden.astype(jnp.float32)
    mean_sq = jnp.mean(wide_h * wide_h, axis=-1, keepdims=True)
    return (wide_h * lax.rsqrt(mean_sq + NORM_EPS) * norm_w.astype(jnp.float32)).astype(jnp.bfloat16)


def reference(hidden, expert_ids, norm_w, router_w, w_gate, w_up, w_down):
    normed = rms_norm(hidden, norm_w)
    logits = jnp.dot(normed, router_w, preferred_element_type=jnp.float32)
    router_prob = jax.nn.softmax(logits, axis=-1)
    gate_prob = jnp.take_along_axis(router_prob, expert_ids, axis=-1).reshape(-1)
    flat_ids = expert_ids.reshape(-1)
    pair_tok = jnp.arange(TOKENS * TOP, dtype=jnp.int32) // TOP
    row_limit = EP * CAP

    def one_expert(accum, per_expert):
        expert, gate_e, up_e, down_e = per_expert
        chosen = flat_ids == expert
        (picked,) = jnp.nonzero(chosen, size=row_limit, fill_value=0)
        row_valid = jnp.arange(row_limit) < jnp.sum(chosen.astype(jnp.int32))
        tok_rows = pair_tok[picked]
        x_rows = normed[tok_rows]
        gate_pre = jnp.dot(x_rows, gate_e, preferred_element_type=jnp.float32)
        up_pre = jnp.dot(x_rows, up_e, preferred_element_type=jnp.float32)
        act_rows = (jax.nn.silu(gate_pre) * up_pre).astype(jnp.bfloat16)
        expert_out = jnp.dot(act_rows, down_e, preferred_element_type=jnp.float32).astype(jnp.bfloat16)
        weight = jnp.where(row_valid, gate_prob[picked], 0.0)
        return accum.at[tok_rows].add(weight[:, None] * expert_out.astype(jnp.float32)), None

    moe_sum, _ = lax.scan(one_expert, jnp.zeros((TOKENS, D), jnp.float32), (jnp.arange(EXPERTS, dtype=jnp.int32), w_gate, w_up, w_down))
    return (hidden.astype(jnp.float32) + moe_sum).astype(jnp.bfloat16)
```

```python
import jax
import jax.numpy as jnp
from jax import lax
from jax.experimental import pallas as pl
from jax.experimental.pallas import tpu as pltpu
from jax.sharding import PartitionSpec as P

NORM_EPS = 1e-6
LANES = 128
BLOCK = 256
PAIR_SLOTS = 10


def moe_kernel(
    hid_hbm, ids_hbm, norm_hbm, router_hbm, gate_hbm, up_hbm, down_hbm, out_hbm,
    w_buf, hid, ids, norm_buf, router, normed, prob_buf, x_buf, act, g3, y_buf,
    part, sib_in, x_out, x_in, y_out, y_in, out_buf,
    w_sem, load_sem, hid_send, hid_recv, ids_send, ids_recv,
    sib_send, sib_recv, xs_sem, xr_sem, ys_sem, yr_sem, out_sem,
):
    me = lax.axis_index("ep")
    tp = lax.axis_index("tp")
    sib = me + 1 - 2 * (me % 2)
    across = (me + 2) % 4
    twin = 1 - tp
    sib_id, across_id, twin_id = {"ep": sib}, {"ep": across}, {"tp": twin}

    tok, dim = hid.shape[1], hid.shape[2]
    n_exp = router.shape[0]
    local_exp = act.shape[0]
    inner = act.shape[2]
    top_k = ids.shape[1]
    cap = x_buf.shape[1] // 4
    n_blocks = dim // BLOCK
    f32, bf16 = jnp.float32, jnp.bfloat16

    def gate_copies(pair):
        slot = pair % PAIR_SLOTS
        return [
            pltpu.make_async_copy(gate_hbm.at[pair], w_buf.at[slot, 0], w_sem.at[slot, 0]),
            pltpu.make_async_copy(up_hbm.at[pair], w_buf.at[slot, 1], w_sem.at[slot, 1]),
        ]

    def down_copy(block, quad):
        slot = (local_exp + block) % PAIR_SLOTS
        rows = 4 * inner
        return pltpu.make_async_copy(
            down_hbm.at[pl.ds(quad * rows, rows), pl.ds(block * BLOCK, BLOCK)],
            w_buf.at[slot, quad // 2, :, pl.ds((quad % 2) * BLOCK, BLOCK)],
            w_sem.at[slot, quad],
        )

    def start_pair(pair):
        if isinstance(pair, int):
            if pair < local_exp:
                for c in gate_copies(pair):
                    c.start()
            elif pair < local_exp + n_blocks:
                for q in range(4):
                    down_copy(pair - local_exp, q).start()
            return

        @pl.when(pair < local_exp)
        def _():
            for c in gate_copies(pair):
                c.start()

        @pl.when((pair >= local_exp) & (pair < local_exp + n_blocks))
        def _():
            for q in range(4):
                down_copy(pair - local_exp, q).start()

    hid_load = pltpu.make_async_copy(hid_hbm, hid.at[0], load_sem.at[0])
    ids_load = pltpu.make_async_copy(ids_hbm, ids.at[0], load_sem.at[1])
    norm_load = pltpu.make_async_copy(norm_hbm, norm_buf, load_sem.at[2])
    router_load = pltpu.make_async_copy(router_hbm, router, load_sem.at[3])
    for c in (hid_load, ids_load, norm_load, router_load):
        c.start()
    for pair in range(PAIR_SLOTS):
        start_pair(pair)

    barrier = pltpu.get_barrier_semaphore()
    for dev in (sib_id, across_id, twin_id):
        pl.semaphore_signal(barrier, inc=1, device_id=dev, device_id_type=pl.DeviceIdType.MESH)
    pl.semaphore_wait(barrier, 3)

    def remote(src, dst, ssem, rsem, dev):
        return pltpu.make_async_remote_copy(
            src_ref=src, dst_ref=dst, send_sem=ssem, recv_sem=rsem,
            device_id=dev, device_id_type=pl.DeviceIdType.MESH,
        )

    def row_copies(j):
        src, dst, dev = ((0, 1, sib_id), (0, 2, across_id), (2, 3, sib_id))[j]
        return (
            remote(hid.at[src], hid.at[dst], hid_send.at[j], hid_recv.at[j], dev),
            remote(ids.at[src], ids.at[dst], ids_send.at[j], ids_recv.at[j], dev),
        )

    hid_load.wait()
    ids_load.wait()
    for j in (1, 0):
        for c in row_copies(j):
            c.start()
    norm_load.wait()
    router_load.wait()

    slot_iota = lax.broadcasted_iota(jnp.int32, (cap, tok), 0).astype(f32)
    exp_iota = lax.broadcasted_iota(jnp.int32, (local_exp, tok), 0) + me * local_exp
    t_row = lax.broadcasted_iota(jnp.int32, (tok, tok), 0)
    t_col = lax.broadcasted_iota(jnp.int32, (tok, tok), 1)
    before = jnp.where(t_row < t_col, 1.0, 0.0).astype(bf16)
    eye = jnp.where(t_row == t_col, 1.0, 0.0).astype(bf16)

    def prepare(k):
        acc = jnp.zeros((tok, LANES), f32)
        for i in range(dim // LANES):
            xs = hid[k, :, pl.ds(i * LANES, LANES)].astype(f32)
            acc = acc + xs * xs
        inv = lax.rsqrt(jnp.sum(acc, axis=1, keepdims=True) / dim + NORM_EPS)
        for i in range(dim // LANES):
            xs = hid[k, :, pl.ds(i * LANES, LANES)].astype(f32)
            w = norm_buf[pl.ds(i, 1), :].astype(f32)
            normed[:, pl.ds(i * LANES, LANES)] = (xs * inv * w).astype(bf16)
        logits = lax.dot_general(router[...], normed[...], (((1,), (1,)), ((), ())), preferred_element_type=f32)
        ex = jnp.exp(logits - jnp.max(logits, axis=0, keepdims=True))
        prob_buf[...] = ex / jnp.sum(ex, axis=0, keepdims=True)
        prob = prob_buf[pl.ds(pl.multiple_of(me * local_exp, local_exp), local_exp), :]
        hit = jnp.zeros((local_exp, tok), f32)
        for j in range(top_k):
            hit = hit + jnp.where(ids[k, pl.ds(j, 1), :] == exp_iota, 1.0, 0.0)
        rank = jnp.dot(hit.astype(bf16), before, preferred_element_type=f32)
        rank = jnp.where(hit > 0.5, rank, -1.0)
        place, weight = [], []
        for e in range(local_exp):
            here = rank[e : e + 1, :] == slot_iota
            place.append(jnp.where(here, 1.0, 0.0))
            weight.append(jnp.where(here, prob[e : e + 1, :], 0.0))
        place = jnp.concatenate(place, axis=0).astype(bf16)
        weight = jnp.concatenate(weight, axis=0)
        for p in range(3):
            piece = weight.astype(bf16)
            if p < 2:
                weight = weight - piece.astype(f32)
            g3[k, pl.ds(p * tok, tok), :] = lax.dot_general(
                eye, piece, (((1,), (1,)), ((), ())), preferred_element_type=f32
            ).astype(bf16)
        for c in range(dim // 512):
            rows = jnp.dot(place, normed[:, pl.ds(c * 512, 512)], preferred_element_type=f32).astype(bf16)
            x_buf[:, pl.ds(k * cap, cap), pl.ds(c * 512, 512)] = rows.reshape(local_exp, cap, 512)

    prepare(0)
    for c in row_copies(0):
        c.wait_recv()
    prepare(1)
    for c in row_copies(1):
        c.wait_recv()
    for c in row_copies(2):
        c.start()
    prepare(2)
    for c in row_copies(2):
        c.wait_recv()
    prepare(3)

    def expert_step(e, carry):
        slot = e % PAIR_SLOTS
        gate_copy, up_copy = gate_copies(e)
        gate_copy.wait()
        gate_pre = jnp.dot(x_buf[e], w_buf[slot, 0], preferred_element_type=f32)
        up_copy.wait()
        up_pre = jnp.dot(x_buf[e], w_buf[slot, 1], preferred_element_type=f32)
        act[e] = (jax.nn.silu(gate_pre) * up_pre).astype(bf16)

        start_pair(e + PAIR_SLOTS)
        return carry

    lax.fori_loop(0, local_exp, expert_step, 0)

    def sib_copies(b):
        return [
            remote(part.at[b, src], sib_in.at[b, i], sib_send.at[b, i], sib_recv.at[b, i], sib_id)
            for i, src in ((1, 3), (0, 1))
        ]

    def x_copy(b):
        return remote(x_out.at[b], x_in.at[b], xs_sem.at[b], xr_sem.at[b], across_id)

    def y_copy(b):
        return remote(y_out.at[b], y_in.at[b], ys_sem.at[b], yr_sem.at[b], twin_id)

    def out_copy(b):
        cols = pl.ds(b * BLOCK, BLOCK)
        return pltpu.make_async_copy(out_buf.at[:, cols], out_hbm.at[:, cols], out_sem.at[b])

    def down_quad(b, q):
        slot = (local_exp + b) % PAIR_SLOTS
        down_copy(b, q).wait()
        for i in range(4):
            e = 4 * q + i
            w = w_buf[slot, q // 2, pl.ds(i * inner, inner), pl.ds((q % 2) * BLOCK, BLOCK)]
            y = jnp.dot(act[e], w, preferred_element_type=f32).astype(bf16)
            for k in range(4):
                y_buf[k, pl.ds(e * cap, cap), :] = y[k * cap : (k + 1) * cap, :]

    def combine(b):
        for k in (3, 1, 2, 0):
            s = jnp.dot(g3[k], y_buf[k], preferred_element_type=f32)
            part[b, k] = s[:tok] + s[tok : 2 * tok] + s[2 * tok :]
            if k == 1:
                for c in sib_copies(b):
                    c.start()

    def stage_x(b):
        first, second = sib_copies(b)
        first.wait_recv()
        x_out[b] = part[b, 2] + sib_in[b, 1]
        x_copy(b).start()
        second.wait_recv()
        y_out[b] = part[b, 0] + sib_in[b, 0]

    def stage_y(b):
        x_copy(b).wait_recv()
        y_out[b] = y_out[b] + x_in[b]
        y_copy(b).start()

    def finish(b):
        y_copy(b).wait_recv()
        cols = pl.ds(b * BLOCK, BLOCK)
        out_buf[:, cols] = (hid[0, :, cols].astype(f32) + (y_out[b] + y_in[b])).astype(bf16)
        out_copy(b).start()

    Y_LAG, OUT_LAG = 4, 7
    for b in range(n_blocks):
        for q in range(4):
            down_quad(b, q)
            if q == 2 and b >= 1:
                stage_x(b - 1)
        combine(b)
        start_pair(local_exp + b + PAIR_SLOTS)
        if b >= Y_LAG:
            stage_y(b - Y_LAG)
        if b >= OUT_LAG:
            finish(b - OUT_LAG)
    stage_x(n_blocks - 1)
    for b in range(n_blocks - Y_LAG, n_blocks):
        stage_y(b)
    for b in range(n_blocks - OUT_LAG, n_blocks):
        finish(b)

    for j in range(3):
        for c in row_copies(j):
            c.wait_send()
    for b in range(n_blocks):
        for c in sib_copies(b):
            c.wait_send()
        x_copy(b).wait_send()
        y_copy(b).wait_send()
        out_copy(b).wait()


def solution(mesh):
    def per_device(hidden, expert_ids, norm_w, router_w, w_gate, w_up, w_down):
        tok, dim = hidden.shape
        top_k = expert_ids.shape[1]
        n_exp = router_w.shape[1]
        local_exp, _, inner = w_gate.shape
        cap = 8 * ((2 * top_k * tok + 8 * n_exp - 1) // (8 * n_exp))
        nb = dim // BLOCK
        f32, bf16 = jnp.float32, jnp.bfloat16
        dma = pltpu.SemaphoreType.DMA
        hbm = pl.BlockSpec(memory_space=pl.ANY)
        return pl.pallas_call(
            moe_kernel,
            out_shape=jax.ShapeDtypeStruct((tok, dim), bf16),
            in_specs=[hbm] * 7,
            out_specs=hbm,
            scratch_shapes=[
                pltpu.VMEM((PAIR_SLOTS, 2, dim, inner), bf16),
                pltpu.VMEM((4, tok, dim), bf16),
                pltpu.VMEM((4, top_k, tok), jnp.int32),
                pltpu.VMEM((dim // LANES, LANES), bf16),
                pltpu.VMEM((n_exp, dim), bf16),
                pltpu.VMEM((tok, dim), bf16),
                pltpu.VMEM((n_exp, tok), f32),
                pltpu.VMEM((local_exp, 4 * cap, dim), bf16),
                pltpu.VMEM((local_exp, 4 * cap, inner), bf16),
                pltpu.VMEM((4, 3 * tok, local_exp * cap), bf16),
                pltpu.VMEM((4, local_exp * cap, BLOCK), bf16),
                pltpu.VMEM((nb, 4, tok, BLOCK), f32),
                pltpu.VMEM((nb, 2, tok, BLOCK), f32),
                pltpu.VMEM((nb, tok, BLOCK), f32),
                pltpu.VMEM((nb, tok, BLOCK), f32),
                pltpu.VMEM((nb, tok, BLOCK), f32),
                pltpu.VMEM((nb, tok, BLOCK), f32),
                pltpu.VMEM((tok, dim), bf16),
                dma((PAIR_SLOTS, 4)),
                dma((4,)),
                dma((3,)), dma((3,)), dma((3,)), dma((3,)),
                dma((nb, 2)), dma((nb, 2)),
                dma((nb,)), dma((nb,)), dma((nb,)), dma((nb,)), dma((nb,)),
            ],
            compiler_params=pltpu.CompilerParams(
                collective_id=0, has_side_effects=True, vmem_limit_bytes=67043328,
            ),
            name="moe",
        )(
            hidden, expert_ids.T, norm_w.reshape(dim // LANES, LANES), router_w.T,
            w_gate, w_up, w_down.reshape(local_exp * inner, dim),
        )

    token_spec = P(("dp", "ep"), None)
    return jax.shard_map(
        per_device, mesh=mesh,
        in_specs=(token_spec, token_spec, P(None), P(None, None), P("ep", None, "tp"), P("ep", None, "tp"), P("ep", "tp", None)),
        out_specs=token_spec, check_vma=False,
    )
```

```python
import jax
import jax.numpy as jnp
from jax import lax
from jax.experimental import pallas as pl
from jax.experimental.pallas import tpu as pltpu
from jax.sharding import PartitionSpec as P

NORM_EPS = 1e-6
LANES = 128
BLOCK = 256
PAIR_SLOTS = 11
BLOCKS = (
    (0, 0, 256, "XR"), (1, 0, 256, "YR"), (2, 0, 256, "YR"), (3, 0, 256, "XR"), (4, 0, 256, "YR"),
    (5, 0, 256, "XR"), (6, 0, 256, "YR"), (7, 0, 256, "X"),
)
STAGES = {"X": 3, "XR": 4, "YR": 4, "D": 2}
LINK, HOP, SIB, MATMULS, ADDS, PIECE, LEAD = 1.52, 2.05, 0.95, 0.78, 0.12, 1.22, 2.0


def static_order():
    x_free = y_free = now = 0.0
    ready, order = {}, []

    def run(b, stage):
        nonlocal x_free, y_free, now
        mode, units = BLOCKS[b][3], LINK * BLOCKS[b][2] / BLOCK
        now = max(now, ready.pop((b, stage))) + ADDS
        order.append(("stage", b, stage))
        if stage + 1 >= STAGES[mode]:
            return
        if mode == "D":
            x_free = max(x_free, now) + 2 * units
            y_free = max(y_free, now) + 2 * units
            then = max(x_free, y_free) + HOP + 0.8
        elif stage < 2 and (stage == 0) == (mode != "YR"):
            then = x_free = max(x_free, now) + (units / 2 if mode == "YR" else units)
            then += HOP
        else:
            share = 0.25 if stage == 2 else 0.5 if mode == "XR" else 1.0
            then = y_free = max(y_free, now) + units * share
            then += HOP
        ready[(b, stage + 1)] = then

    for b, (piece, first, width, _) in enumerate(BLOCKS):
        arrive = PIECE * (piece + (first + width) / BLOCK) - LEAD
        while ready:
            key = min(ready, key=ready.get)
            if ready[key] > now and ready[key] + ADDS > arrive:
                break
            run(*key)
        now = max(now, arrive) + MATMULS
        order.append(("block", b, 0))
        ready[(b, 0)] = now + SIB
    while ready:
        run(*min(ready, key=ready.get))
    return order


def moe_kernel(
    hid_hbm, ids_hbm, norm_hbm, router_hbm, gate_hbm, up_hbm, down_hbm, out,
    w_buf, hid, ids, norm_buf, router, normed, prob_buf, x_buf, act, g3, y_buf,
    part, sib_in, x_out, x_in, y_out, y_in, z_in, fin, fin_in,
    w_sem, load_sem, hid_send, hid_recv, ids_send, ids_recv,
    sib_send, sib_recv, xs_sem, xr_sem, ys_sem, yr_sem, zs_sem, zr_sem, fs_sem, fr_sem,
):
    me = lax.axis_index("ep")
    tp = lax.axis_index("tp")
    sib = me + 1 - 2 * (me % 2)
    across = (me + 2) % 4
    twin = 1 - tp
    sib_id, across_id, twin_id, diag_id = {"ep": sib}, {"ep": across}, {"tp": twin}, {"ep": across, "tp": twin}

    tok, dim = hid.shape[1], hid.shape[2]
    n_exp = router.shape[0]
    local_exp = act.shape[0]
    inner = act.shape[2]
    top_k = ids.shape[1]
    cap = x_buf.shape[1] // 4
    n_pieces = dim // BLOCK
    f32, bf16 = jnp.float32, jnp.bfloat16

    def gate_copies(pair):
        slot = pair % PAIR_SLOTS
        return [
            pltpu.make_async_copy(gate_hbm.at[pair], w_buf.at[slot, 0], w_sem.at[slot, 0]),
            pltpu.make_async_copy(up_hbm.at[pair], w_buf.at[slot, 1], w_sem.at[slot, 1]),
        ]

    def down_copy(piece, quad, first, width):
        slot = (local_exp + piece) % PAIR_SLOTS
        rows = 4 * inner
        return pltpu.make_async_copy(
            down_hbm.at[pl.ds(quad * rows, rows), pl.ds(piece * BLOCK + first, width)],
            w_buf.at[slot, quad // 2, :, pl.ds((quad % 2) * BLOCK + first, width)],
            w_sem.at[slot, quad + 4 * (first // LANES)],
        )

    def start_pair(pair):
        if pair < local_exp:
            for c in gate_copies(pair):
                c.start(priority=1)
        elif pair < local_exp + n_pieces:
            for piece, first, width, _ in BLOCKS:
                if piece == pair - local_exp:
                    for q in range(4):
                        down_copy(piece, q, first, width).start(priority=1)

    hid_load = pltpu.make_async_copy(hid_hbm, hid.at[0], load_sem.at[0])
    ids_load = pltpu.make_async_copy(ids_hbm, ids.at[0], load_sem.at[1])
    norm_load = pltpu.make_async_copy(norm_hbm, norm_buf, load_sem.at[2])
    router_load = pltpu.make_async_copy(router_hbm, router, load_sem.at[3])
    for c in (hid_load, ids_load, norm_load, router_load):
        c.start()
    for pair in range(PAIR_SLOTS):
        start_pair(pair)

    barrier = pltpu.get_barrier_semaphore()
    for dev in (sib_id, across_id, twin_id, diag_id):
        pl.semaphore_signal(barrier, inc=1, device_id=dev, device_id_type=pl.DeviceIdType.MESH)
    pl.semaphore_wait(barrier, 4)

    def remote(src, dst, ssem, rsem, dev):
        return pltpu.make_async_remote_copy(
            src_ref=src, dst_ref=dst, send_sem=ssem, recv_sem=rsem,
            device_id=dev, device_id_type=pl.DeviceIdType.MESH,
        )

    def row_copies(j):
        src, dst, dev = ((0, 1, sib_id), (0, 2, across_id), (2, 3, sib_id))[j]
        return (
            remote(hid.at[src], hid.at[dst], hid_send.at[j], hid_recv.at[j], dev),
            remote(ids.at[src], ids.at[dst], ids_send.at[j], ids_recv.at[j], dev),
        )

    hid_load.wait()
    ids_load.wait()
    for j in (1, 0):
        for c in row_copies(j):
            c.start()
    norm_load.wait()
    router_load.wait()

    slot_iota = lax.broadcasted_iota(jnp.int32, (cap, tok), 0).astype(f32)
    exp_iota = lax.broadcasted_iota(jnp.int32, (local_exp, tok), 0) + me * local_exp
    t_row = lax.broadcasted_iota(jnp.int32, (tok, tok), 0)
    t_col = lax.broadcasted_iota(jnp.int32, (tok, tok), 1)
    before = jnp.where(t_row < t_col, 1.0, 0.0).astype(bf16)
    eye = jnp.where(t_row == t_col, 1.0, 0.0).astype(bf16)

    def prepare(k):
        acc = jnp.zeros((tok, LANES), f32)
        for i in range(dim // LANES):
            xs = hid[k, :, pl.ds(i * LANES, LANES)].astype(f32)
            acc = acc + xs * xs
        inv = lax.rsqrt(jnp.sum(acc, axis=1, keepdims=True) / dim + NORM_EPS)
        for i in range(dim // LANES):
            xs = hid[k, :, pl.ds(i * LANES, LANES)].astype(f32)
            w = norm_buf[pl.ds(i, 1), :].astype(f32)
            normed[:, pl.ds(i * LANES, LANES)] = (xs * inv * w).astype(bf16)
        logits = lax.dot_general(router[...], normed[...], (((1,), (1,)), ((), ())), preferred_element_type=f32)
        ex = jnp.exp(logits - jnp.max(logits, axis=0, keepdims=True))
        prob_buf[...] = ex / jnp.sum(ex, axis=0, keepdims=True)
        prob = prob_buf[pl.ds(pl.multiple_of(me * local_exp, local_exp), local_exp), :]
        hit = jnp.zeros((local_exp, tok), f32)
        for j in range(top_k):
            hit = hit + jnp.where(ids[k, pl.ds(j, 1), :] == exp_iota, 1.0, 0.0)
        rank = jnp.dot(hit.astype(bf16), before, preferred_element_type=f32)
        rank = jnp.where(hit > 0.5, rank, -1.0)
        place, weight = [], []
        for e in range(local_exp):
            here = rank[e : e + 1, :] == slot_iota
            place.append(jnp.where(here, 1.0, 0.0))
            weight.append(jnp.where(here, prob[e : e + 1, :], 0.0))
        place = jnp.concatenate(place, axis=0).astype(bf16)
        weight = jnp.concatenate(weight, axis=0)
        for p in range(3):
            piece = weight.astype(bf16)
            if p < 2:
                weight = weight - piece.astype(f32)
            g3[k, pl.ds(p * tok, tok), :] = lax.dot_general(
                eye, piece, (((1,), (1,)), ((), ())), preferred_element_type=f32
            ).astype(bf16)
        for c in range(dim // 512):
            rows = jnp.dot(place, normed[:, pl.ds(c * 512, 512)], preferred_element_type=f32).astype(bf16)
            x_buf[:, pl.ds(k * cap, cap), pl.ds(c * 512, 512)] = rows.reshape(local_exp, cap, 512)

    prepare(0)
    for c in row_copies(0):
        c.wait_recv()
    prepare(1)
    for c in row_copies(1):
        c.wait_recv()
    for c in row_copies(2):
        c.start()
    prepare(2)
    for c in row_copies(2):
        c.wait_recv()
    prepare(3)

    def twice(rows):
        return jnp.concatenate([rows, rows], axis=0)

    def experts(first, count):
        for i in range(count):
            for c in gate_copies(first + i):
                c.wait()
        for i in range(count):
            e = first + i
            slot = e % PAIR_SLOTS
            x = twice(x_buf[e])
            gate_pre = jnp.dot(x, w_buf[slot, 0], preferred_element_type=f32)[: 4 * cap]
            up_pre = jnp.dot(x, w_buf[slot, 1], preferred_element_type=f32)[: 4 * cap]
            act[e] = (jax.nn.silu(gate_pre) * up_pre).astype(bf16)

    more_pairs = local_exp - PAIR_SLOTS

    def expert_step(i, carry):
        experts(i, 1)
        for c in gate_copies(i + PAIR_SLOTS):
            c.start(priority=1)
        return carry

    lax.fori_loop(0, more_pairs, expert_step, 0)
    for e in range(more_pairs, local_exp):
        experts(e, 1)
        start_pair(e + PAIR_SLOTS)

    def cols_of(b):
        piece, first, width, _ = BLOCKS[b]
        return piece * BLOCK + first, width

    def sib_copies(b):
        w = pl.ds(0, BLOCKS[b][2])
        return [
            remote(part.at[b, src, :, w], sib_in.at[b, i, :, w], sib_send.at[b, i], sib_recv.at[b, i], sib_id)
            for i, src in ((1, 3), (0, 1))
        ]

    def lanes(b, which):
        w = BLOCKS[b][2]
        if which == "all":
            return pl.ds(0, w)
        return pl.ds(pl.multiple_of((tp if which == "mine" else twin) * (w // 2), LANES), w // 2)

    def x_copy(b):
        w = lanes(b, "mine" if BLOCKS[b][3] == "YR" else "all")
        return remote(x_out.at[b, :, w], x_in.at[b, :, w], xs_sem.at[b], xr_sem.at[b], across_id)

    def y_copy(b):
        w = lanes(b, "theirs" if BLOCKS[b][3] in ("XR", "YR") else "all")
        return remote(y_out.at[b, :, w], y_in.at[b, :, w], ys_sem.at[b], yr_sem.at[b], twin_id)

    def z_copy(b):
        yr = BLOCKS[b][3] == "YR"
        w = lanes(b, "theirs" if yr else "all")
        return remote(x_out.at[b, :, w], z_in.at[b, :, w], zs_sem.at[b], zr_sem.at[b], twin_id if yr else diag_id)

    def fin_copy(b):
        return remote(fin.at[b], fin_in.at[b], fs_sem.at[b], fr_sem.at[b], twin_id)

    def compute(b):
        piece, first, width, _ = BLOCKS[b]
        slot = (local_exp + piece) % PAIR_SLOTS
        for q in range(4):
            down_copy(piece, q, first, width).wait()
        for q in range(4):
            for i in range(4):
                e = 4 * q + i
                w = w_buf[slot, q // 2, pl.ds(i * inner, inner), pl.ds((q % 2) * BLOCK + first, width)]
                y = jnp.dot(twice(act[e]), w, preferred_element_type=f32)[: 4 * cap].astype(bf16)
                for k in range(4):
                    y_buf[k, pl.ds(e * cap, cap), pl.ds(0, width)] = y[k * cap : (k + 1) * cap, :]
        for k in (3, 1, 2, 0):
            s = jnp.dot(g3[k], y_buf[k, :, pl.ds(0, width)], preferred_element_type=f32)
            part[b, k, :, pl.ds(0, width)] = s[:tok] + s[tok : 2 * tok] + s[2 * tok :]
            if k == 1:
                for c in sib_copies(b):
                    c.start()

    def put(b, which, value):
        start, width = cols_of(b)
        if which == "all":
            cols = pl.ds(start, width)
        else:
            half = width // 2
            cols = pl.ds(pl.multiple_of(start + (tp if which == "mine" else twin) * half, LANES), half)
        if which == "theirs":
            out[:, cols] = value
            return None
        result = (hid[0, :, cols].astype(f32) + value).astype(bf16)
        out[:, cols] = result
        return result

    def stage(b, n):
        mode = BLOCKS[b][3]
        full, mine = lanes(b, "all"), lanes(b, "mine") if mode in ("XR", "YR") else None
        if n == 0:
            first, second = sib_copies(b)
            first.wait_recv()
            x_out[b, :, full] = part[b, 2, :, full] + sib_in[b, 1, :, full]
            (z_copy if mode == "YR" else x_copy)(b).start()
            if mode == "D":
                z_copy(b).start()
            second.wait_recv()
            y_out[b, :, full] = part[b, 0, :, full] + sib_in[b, 0, :, full]
            if mode in ("YR", "D"):
                y_copy(b).start()
        elif mode == "D":
            x_copy(b).wait_recv()
            y_copy(b).wait_recv()
            z_copy(b).wait_recv()
            put(b, "all", (y_out[b, :, full] + x_in[b, :, full]) + (y_in[b, :, full] + z_in[b, :, full]))
        elif n == 1 and mode == "YR":
            z_copy(b).wait_recv()
            x_out[b, :, mine] = x_out[b, :, mine] + z_in[b, :, mine]
            x_copy(b).start()
            y_copy(b).wait_recv()
            y_out[b, :, mine] = y_out[b, :, mine] + y_in[b, :, mine]
        elif n == 1:
            x_copy(b).wait_recv()
            y_out[b, :, full] = y_out[b, :, full] + x_in[b, :, full]
            y_copy(b).start()
        elif mode == "X":
            y_copy(b).wait_recv()
            put(b, "all", y_out[b, :, full] + y_in[b, :, full])
        elif n == 2:
            (x_copy if mode == "YR" else y_copy)(b).wait_recv()
            other = x_in if mode == "YR" else y_in
            fin[b] = put(b, "mine", y_out[b, :, mine] + other[b, :, mine])
            fin_copy(b).start()
        else:
            fin_copy(b).wait_recv()
            put(b, "theirs", fin_in[b])

    for kind, b, n in static_order():
        if kind == "block":
            compute(b)
        else:
            stage(b, n)

    for j in range(3):
        for c in row_copies(j):
            c.wait_send()
    for b, (_, _, _, mode) in enumerate(BLOCKS):
        for c in sib_copies(b):
            c.wait_send()
        x_copy(b).wait_send()
        y_copy(b).wait_send()
        if mode in ("YR", "D"):
            z_copy(b).wait_send()
        if mode in ("YR", "XR"):
            fin_copy(b).wait_send()


def solution(mesh):
    def per_device(hidden, expert_ids, norm_w, router_w, w_gate, w_up, w_down):
        tok, dim = hidden.shape
        top_k = expert_ids.shape[1]
        n_exp = router_w.shape[1]
        local_exp, _, inner = w_gate.shape
        cap = 8 * ((2 * top_k * tok + 8 * n_exp - 1) // (8 * n_exp))
        nb = len(BLOCKS)
        f32, bf16 = jnp.float32, jnp.bfloat16
        dma = pltpu.SemaphoreType.DMA
        hbm = pl.BlockSpec(memory_space=pl.ANY)
        return pl.pallas_call(
            moe_kernel,
            out_shape=pltpu.VMEM((tok, dim), bf16),
            in_specs=[hbm] * 7,
            out_specs=pl.BlockSpec(memory_space=pltpu.VMEM),
            scratch_shapes=[
                pltpu.VMEM((PAIR_SLOTS, 2, dim, inner), bf16),
                pltpu.VMEM((4, tok, dim), bf16),
                pltpu.VMEM((4, top_k, tok), jnp.int32),
                pltpu.VMEM((dim // LANES, LANES), bf16),
                pltpu.VMEM((n_exp, dim), bf16),
                pltpu.VMEM((tok, dim), bf16),
                pltpu.VMEM((n_exp, tok), f32),
                pltpu.VMEM((local_exp, 4 * cap, dim), bf16),
                pltpu.VMEM((local_exp, 4 * cap, inner), bf16),
                pltpu.VMEM((4, 3 * tok, local_exp * cap), bf16),
                pltpu.VMEM((4, local_exp * cap, BLOCK), bf16),
                pltpu.VMEM((nb, 4, tok, BLOCK), f32),
                pltpu.VMEM((nb, 2, tok, BLOCK), f32),
                pltpu.VMEM((nb, tok, BLOCK), f32),
                pltpu.VMEM((nb, tok, BLOCK), f32),
                pltpu.VMEM((nb, tok, BLOCK), f32),
                pltpu.VMEM((nb, tok, BLOCK), f32),
                pltpu.VMEM((nb, tok, BLOCK), f32),
                pltpu.VMEM((nb, tok, LANES), bf16),
                pltpu.VMEM((nb, tok, LANES), bf16),
                dma((PAIR_SLOTS, 8)),
                dma((4,)),
                dma((3,)), dma((3,)), dma((3,)), dma((3,)),
                dma((nb, 2)), dma((nb, 2)),
                *[dma((nb,))] * 8,
            ],
            compiler_params=pltpu.CompilerParams(
                collective_id=0, has_side_effects=True, vmem_limit_bytes=62 * 2**20,
            ),
            name="moe",
        )(
            hidden, expert_ids.T, norm_w.reshape(dim // LANES, LANES), router_w.T,
            w_gate, w_up, w_down.reshape(local_exp * inner, dim),
        )

    token_spec = P(("dp", "ep"), None)
    return jax.shard_map(
        per_device, mesh=mesh,
        in_specs=(token_spec, token_spec, P(None), P(None, None), P("ep", None, "tp"), P("ep", None, "tp"), P("ep", "tp", None)),
        out_specs=token_spec, check_vma=False,
    )
```

```python
import jax
import jax.numpy as jnp
from jax import lax
from jax.experimental import pallas as pl
from jax.experimental.pallas import tpu as pltpu
from jax.sharding import PartitionSpec as P

NORM_EPS = 1e-6
LANES = 128
BLOCK = 256
PAIR_SLOTS = 11
BLOCKS = (
    (0, 0, 256, "X"), (1, 0, 256, "YR"), (2, 0, 256, "YR"), (3, 0, 256, "XR"), (4, 0, 256, "YR"),
    (5, 0, 256, "X"), (6, 0, 256, "YR"), (7, 0, 256, "X"),
)
STAGES = {"X": 3, "XR": 4, "YR": 4}
LINK, HOP, SIB, MATMULS, ADDS, PIECE, LEAD = 1.52, 2.05, 0.95, 0.78, 0.12, 1.22, 0.8


def static_order():
    x_free = y_free = now = 0.0
    ready, order = {}, []

    def run(b, stage):
        nonlocal x_free, y_free, now
        mode, units = BLOCKS[b][3], LINK * BLOCKS[b][2] / BLOCK
        now = max(now, ready.pop((b, stage))) + ADDS
        order.append(("stage", b, stage))
        if stage + 1 >= STAGES[mode]:
            return
        if stage < 2 and (stage == 0) == (mode != "YR"):
            then = x_free = max(x_free, now) + (units / 2 if mode == "YR" else units)
            then += HOP
        else:
            share = 0.25 if stage == 2 else 0.5 if mode == "XR" else 1.0
            then = y_free = max(y_free, now) + units * share
            then += HOP
        ready[(b, stage + 1)] = then

    for b, (piece, first, width, _) in enumerate(BLOCKS):
        arrive = PIECE * (piece + (first + width) / BLOCK) - LEAD
        while ready:
            key = min(ready, key=ready.get)
            if ready[key] > now and ready[key] + ADDS > arrive:
                break
            run(*key)
        now = max(now, arrive) + MATMULS
        order.append(("block", b, 0))
        ready[(b, 0)] = now + SIB
    while ready:
        run(*min(ready, key=ready.get))
    return order


def moe_kernel(
    hid_hbm, ids_hbm, norm_hbm, router_hbm, gate_hbm, up_hbm, down_hbm, out,
    w_buf, hid, ids, norm_buf, router, normed, prob_buf, x_buf, act, g3, y_buf,
    part, sib_in, x_out, x_in, y_out, y_in, z_in, fin, fin_in,
    w_sem, load_sem, hid_send, hid_recv, ids_send, ids_recv,
    sib_send, sib_recv, xs_sem, xr_sem, ys_sem, yr_sem, zs_sem, zr_sem, fs_sem, fr_sem,
):
    me = lax.axis_index("ep")
    tp = lax.axis_index("tp")
    sib = me + 1 - 2 * (me % 2)
    across = (me + 2) % 4
    twin = 1 - tp
    sib_id, across_id, twin_id = {"ep": sib}, {"ep": across}, {"tp": twin}

    tok, dim = hid.shape[1], hid.shape[2]
    n_exp = router.shape[0]
    local_exp = act.shape[0]
    inner = act.shape[2]
    top_k = ids.shape[1]
    cap = x_buf.shape[1] // 4
    n_pieces = dim // BLOCK
    f32, bf16 = jnp.float32, jnp.bfloat16

    def gate_copies(pair):
        slot = pair % PAIR_SLOTS
        return [
            pltpu.make_async_copy(gate_hbm.at[pair], w_buf.at[slot, 0], w_sem.at[slot, 0]),
            pltpu.make_async_copy(up_hbm.at[pair], w_buf.at[slot, 1], w_sem.at[slot, 1]),
        ]

    def down_copy(piece, quad, first, width):
        slot = (local_exp + piece) % PAIR_SLOTS
        rows = 4 * inner
        return pltpu.make_async_copy(
            down_hbm.at[pl.ds(quad * rows, rows), pl.ds(piece * BLOCK + first, width)],
            w_buf.at[slot, quad // 2, :, pl.ds((quad % 2) * BLOCK + first, width)],
            w_sem.at[slot, quad + 4 * (first // LANES)],
        )

    def start_pair(pair):
        if pair < local_exp:
            for c in gate_copies(pair):
                c.start(priority=1)
        elif pair < local_exp + n_pieces:
            for piece, first, width, _ in BLOCKS:
                if piece == pair - local_exp:
                    for q in range(4):
                        down_copy(piece, q, first, width).start(priority=1)

    hid_load = pltpu.make_async_copy(hid_hbm, hid.at[0], load_sem.at[0])
    ids_load = pltpu.make_async_copy(ids_hbm, ids.at[0], load_sem.at[1])
    norm_load = pltpu.make_async_copy(norm_hbm, norm_buf, load_sem.at[2])
    router_load = pltpu.make_async_copy(router_hbm, router, load_sem.at[3])
    for c in (hid_load, ids_load, norm_load, router_load):
        c.start()
    for pair in range(PAIR_SLOTS):
        start_pair(pair)

    barrier = pltpu.get_barrier_semaphore()
    for dev in (sib_id, across_id, twin_id):
        pl.semaphore_signal(barrier, inc=1, device_id=dev, device_id_type=pl.DeviceIdType.MESH)
    pl.semaphore_wait(barrier, 3)

    def remote(src, dst, ssem, rsem, dev):
        return pltpu.make_async_remote_copy(
            src_ref=src, dst_ref=dst, send_sem=ssem, recv_sem=rsem,
            device_id=dev, device_id_type=pl.DeviceIdType.MESH,
        )

    def row_copies(j):
        src, dst, dev = ((0, 1, sib_id), (0, 2, across_id), (2, 3, sib_id))[j]
        return (
            remote(hid.at[src], hid.at[dst], hid_send.at[j], hid_recv.at[j], dev),
            remote(ids.at[src], ids.at[dst], ids_send.at[j], ids_recv.at[j], dev),
        )

    hid_load.wait()
    ids_load.wait()
    for j in (1, 0):
        for c in row_copies(j):
            c.start()
    norm_load.wait()
    router_load.wait()

    slot_iota = lax.broadcasted_iota(jnp.int32, (cap, tok), 0).astype(f32)
    exp_iota = lax.broadcasted_iota(jnp.int32, (local_exp, tok), 0) + me * local_exp
    t_row = lax.broadcasted_iota(jnp.int32, (tok, tok), 0)
    t_col = lax.broadcasted_iota(jnp.int32, (tok, tok), 1)
    before = jnp.where(t_row < t_col, 1.0, 0.0).astype(bf16)
    eye = jnp.where(t_row == t_col, 1.0, 0.0).astype(bf16)

    def prepare(k):
        acc = jnp.zeros((tok, LANES), f32)
        for i in range(dim // LANES):
            xs = hid[k, :, pl.ds(i * LANES, LANES)].astype(f32)
            acc = acc + xs * xs
        inv = lax.rsqrt(jnp.sum(acc, axis=1, keepdims=True) / dim + NORM_EPS)
        for i in range(dim // LANES):
            xs = hid[k, :, pl.ds(i * LANES, LANES)].astype(f32)
            w = norm_buf[pl.ds(i, 1), :].astype(f32)
            normed[:, pl.ds(i * LANES, LANES)] = (xs * inv * w).astype(bf16)
        logits = lax.dot_general(router[...], normed[...], (((1,), (1,)), ((), ())), preferred_element_type=f32)
        ex = jnp.exp(logits - jnp.max(logits, axis=0, keepdims=True))
        prob_buf[...] = ex / jnp.sum(ex, axis=0, keepdims=True)
        prob = prob_buf[pl.ds(pl.multiple_of(me * local_exp, local_exp), local_exp), :]
        hit = jnp.zeros((local_exp, tok), f32)
        for j in range(top_k):
            hit = hit + jnp.where(ids[k, pl.ds(j, 1), :] == exp_iota, 1.0, 0.0)
        rank = jnp.dot(hit.astype(bf16), before, preferred_element_type=f32)
        rank = jnp.where(hit > 0.5, rank, -1.0)
        place, weight = [], []
        for e in range(local_exp):
            here = rank[e : e + 1, :] == slot_iota
            place.append(jnp.where(here, 1.0, 0.0))
            weight.append(jnp.where(here, prob[e : e + 1, :], 0.0))
        place = jnp.concatenate(place, axis=0).astype(bf16)
        weight = jnp.concatenate(weight, axis=0)
        for p in range(3):
            piece = weight.astype(bf16)
            if p < 2:
                weight = weight - piece.astype(f32)
            g3[k, pl.ds(p * tok, tok), :] = lax.dot_general(
                eye, piece, (((1,), (1,)), ((), ())), preferred_element_type=f32
            ).astype(bf16)
        for c in range(dim // 512):
            rows = jnp.dot(place, normed[:, pl.ds(c * 512, 512)], preferred_element_type=f32).astype(bf16)
            x_buf[:, pl.ds(k * cap, cap), pl.ds(c * 512, 512)] = rows.reshape(local_exp, cap, 512)

    prepare(0)
    for c in row_copies(0):
        c.wait_recv()
    prepare(1)
    for c in row_copies(1):
        c.wait_recv()
    for c in row_copies(2):
        c.start()
    prepare(2)
    for c in row_copies(2):
        c.wait_recv()
    prepare(3)

    def twice(rows):
        return jnp.concatenate([rows, rows], axis=0)

    def experts(first, count):
        for i in range(count):
            for c in gate_copies(first + i):
                c.wait()
        for i in range(count):
            e = first + i
            slot = e % PAIR_SLOTS
            x = twice(x_buf[e])
            gate_pre = jnp.dot(x, w_buf[slot, 0], preferred_element_type=f32)[: 4 * cap]
            up_pre = jnp.dot(x, w_buf[slot, 1], preferred_element_type=f32)[: 4 * cap]
            act[e] = (jax.nn.silu(gate_pre) * up_pre).astype(bf16)

    more_pairs = (local_exp - PAIR_SLOTS) // 2

    def expert_step(i, carry):
        experts(2 * i, 2)
        for j in range(2):
            for c in gate_copies(2 * i + j + PAIR_SLOTS):
                c.start(priority=1)
        return carry

    lax.fori_loop(0, more_pairs, expert_step, 0)
    e = 2 * more_pairs
    while e < local_exp:
        count = 2 if e < local_exp - 2 else 1
        experts(e, count)
        for j in range(count):
            start_pair(e + j + PAIR_SLOTS)
        e += count

    def cols_of(b):
        piece, first, width, _ = BLOCKS[b]
        return piece * BLOCK + first, width

    def sib_copies(b):
        w = pl.ds(0, BLOCKS[b][2])
        return [
            remote(part.at[b, src, :, w], sib_in.at[b, i, :, w], sib_send.at[b, i], sib_recv.at[b, i], sib_id)
            for i, src in ((1, 3), (0, 1))
        ]

    def lanes(b, which):
        w = BLOCKS[b][2]
        if which == "all":
            return pl.ds(0, w)
        return pl.ds(pl.multiple_of((tp if which == "mine" else twin) * (w // 2), LANES), w // 2)

    def x_copy(b):
        w = lanes(b, "mine" if BLOCKS[b][3] == "YR" else "all")
        return remote(x_out.at[b, :, w], x_in.at[b, :, w], xs_sem.at[b], xr_sem.at[b], across_id)

    def y_copy(b):
        w = lanes(b, "theirs" if BLOCKS[b][3] in ("XR", "YR") else "all")
        return remote(y_out.at[b, :, w], y_in.at[b, :, w], ys_sem.at[b], yr_sem.at[b], twin_id)

    def z_copy(b):
        w = lanes(b, "theirs")
        return remote(x_out.at[b, :, w], z_in.at[b, :, w], zs_sem.at[b], zr_sem.at[b], twin_id)

    def fin_copy(b):
        return remote(fin.at[b], fin_in.at[b], fs_sem.at[b], fr_sem.at[b], twin_id)

    def compute(b):
        piece, first, width, _ = BLOCKS[b]
        slot = (local_exp + piece) % PAIR_SLOTS
        for q in range(4):
            down_copy(piece, q, first, width).wait()
        for q in range(4):
            for i in range(4):
                e = 4 * q + i
                w = w_buf[slot, q // 2, pl.ds(i * inner, inner), pl.ds((q % 2) * BLOCK + first, width)]
                y = jnp.dot(twice(act[e]), w, preferred_element_type=f32)[: 4 * cap].astype(bf16)
                for k in range(4):
                    y_buf[k, pl.ds(e * cap, cap), pl.ds(0, width)] = y[k * cap : (k + 1) * cap, :]
        for k in (3, 1, 2, 0):
            s = jnp.dot(g3[k], y_buf[k, :, pl.ds(0, width)], preferred_element_type=f32)
            part[b, k, :, pl.ds(0, width)] = s[:tok] + s[tok : 2 * tok] + s[2 * tok :]
            if k == 1:
                for c in sib_copies(b):
                    c.start()

    def put(b, which, value):
        start, width = cols_of(b)
        if which == "all":
            cols = pl.ds(start, width)
        else:
            half = width // 2
            cols = pl.ds(pl.multiple_of(start + (tp if which == "mine" else twin) * half, LANES), half)
        if which == "theirs":
            out[:, cols] = value
            return None
        result = (hid[0, :, cols].astype(f32) + value).astype(bf16)
        out[:, cols] = result
        return result

    def stage(b, n):
        mode = BLOCKS[b][3]
        full, mine = lanes(b, "all"), lanes(b, "mine") if mode in ("XR", "YR") else None
        if n == 0:
            first, second = sib_copies(b)
            first.wait_recv()
            x_out[b, :, full] = part[b, 2, :, full] + sib_in[b, 1, :, full]
            (z_copy if mode == "YR" else x_copy)(b).start()
            second.wait_recv()
            y_out[b, :, full] = part[b, 0, :, full] + sib_in[b, 0, :, full]
            if mode == "YR":
                y_copy(b).start()
        elif n == 1 and mode == "YR":
            z_copy(b).wait_recv()
            x_out[b, :, mine] = x_out[b, :, mine] + z_in[b, :, mine]
            x_copy(b).start()
            y_copy(b).wait_recv()
            y_out[b, :, mine] = y_out[b, :, mine] + y_in[b, :, mine]
        elif n == 1:
            x_copy(b).wait_recv()
            y_out[b, :, full] = y_out[b, :, full] + x_in[b, :, full]
            y_copy(b).start()
        elif mode == "X":
            y_copy(b).wait_recv()
            put(b, "all", y_out[b, :, full] + y_in[b, :, full])
        elif n == 2:
            (x_copy if mode == "YR" else y_copy)(b).wait_recv()
            other = x_in if mode == "YR" else y_in
            fin[b] = put(b, "mine", y_out[b, :, mine] + other[b, :, mine])
            fin_copy(b).start()
        else:
            fin_copy(b).wait_recv()
            put(b, "theirs", fin_in[b])

    for kind, b, n in static_order():
        if kind == "block":
            compute(b)
        else:
            stage(b, n)

    for j in range(3):
        for c in row_copies(j):
            c.wait_send()
    for b, (_, _, _, mode) in enumerate(BLOCKS):
        for c in sib_copies(b):
            c.wait_send()
        x_copy(b).wait_send()
        y_copy(b).wait_send()
        if mode == "YR":
            z_copy(b).wait_send()
        if mode in ("YR", "XR"):
            fin_copy(b).wait_send()


def solution(mesh):
    def per_device(hidden, expert_ids, norm_w, router_w, w_gate, w_up, w_down):
        tok, dim = hidden.shape
        top_k = expert_ids.shape[1]
        n_exp = router_w.shape[1]
        local_exp, _, inner = w_gate.shape
        cap = 8 * ((2 * top_k * tok + 8 * n_exp - 1) // (8 * n_exp))
        nb = len(BLOCKS)
        f32, bf16 = jnp.float32, jnp.bfloat16
        dma = pltpu.SemaphoreType.DMA
        hbm = pl.BlockSpec(memory_space=pl.ANY)
        return pl.pallas_call(
            moe_kernel,
            out_shape=pltpu.VMEM((tok, dim), bf16),
            in_specs=[hbm] * 7,
            out_specs=pl.BlockSpec(memory_space=pltpu.VMEM),
            scratch_shapes=[
                pltpu.VMEM((PAIR_SLOTS, 2, dim, inner), bf16),
                pltpu.VMEM((4, tok, dim), bf16),
                pltpu.VMEM((4, top_k, tok), jnp.int32),
                pltpu.VMEM((dim // LANES, LANES), bf16),
                pltpu.VMEM((n_exp, dim), bf16),
                pltpu.VMEM((tok, dim), bf16),
                pltpu.VMEM((n_exp, tok), f32),
                pltpu.VMEM((local_exp, 4 * cap, dim), bf16),
                pltpu.VMEM((local_exp, 4 * cap, inner), bf16),
                pltpu.VMEM((4, 3 * tok, local_exp * cap), bf16),
                pltpu.VMEM((4, local_exp * cap, BLOCK), bf16),
                pltpu.VMEM((nb, 4, tok, BLOCK), f32),
                pltpu.VMEM((nb, 2, tok, BLOCK), f32),
                pltpu.VMEM((nb, tok, BLOCK), f32),
                pltpu.VMEM((nb, tok, BLOCK), f32),
                pltpu.VMEM((nb, tok, BLOCK), f32),
                pltpu.VMEM((nb, tok, BLOCK), f32),
                pltpu.VMEM((nb, tok, BLOCK), f32),
                pltpu.VMEM((nb, tok, LANES), bf16),
                pltpu.VMEM((nb, tok, LANES), bf16),
                dma((PAIR_SLOTS, 8)),
                dma((4,)),
                dma((3,)), dma((3,)), dma((3,)), dma((3,)),
                dma((nb, 2)), dma((nb, 2)),
                *[dma((nb,))] * 8,
            ],
            compiler_params=pltpu.CompilerParams(
                collective_id=0, has_side_effects=True, vmem_limit_bytes=62 * 2**20,
            ),
            name="moe",
        )(
            hidden, expert_ids.T, norm_w.reshape(dim // LANES, LANES), router_w.T,
            w_gate, w_up, w_down.reshape(local_exp * inner, dim),
        )

    token_spec = P(("dp", "ep"), None)
    return jax.shard_map(
        per_device, mesh=mesh,
        in_specs=(token_spec, token_spec, P(None), P(None, None), P("ep", None, "tp"), P("ep", None, "tp"), P("ep", "tp", None)),
        out_specs=token_spec, check_vma=False,
    )
```

```python
import jax
import jax.numpy as jnp
from jax import lax
from jax.experimental import pallas as pl
from jax.experimental.pallas import tpu as pltpu
from jax.sharding import PartitionSpec as P

NORM_EPS = 1e-6
LANES = 128
BLOCK = 256
PAIR_SLOTS = 11
BLOCKS = (
    (0, 0, 256, "X"), (1, 0, 256, "XR"), (2, 0, 256, "YR"), (3, 0, 256, "XR"), (4, 0, 256, "X"),
    (5, 0, 256, "YR"), (6, 0, 256, "X"), (7, 0, 256, "X"),
)
STAGES = {"X": 3, "XR": 4, "YR": 4}
LINK, HOP, SIB, MATMULS, ADDS, PIECE, LEAD = 1.52, 2.05, 0.95, 0.9, 0.12, 1.3, 0.0


def static_order():
    x_free = y_free = now = 0.0
    ready, order = {}, []

    def run(b, stage):
        nonlocal x_free, y_free, now
        mode, units = BLOCKS[b][3], LINK * BLOCKS[b][2] / BLOCK
        now = max(now, ready.pop((b, stage))) + ADDS
        order.append(("stage", b, stage))
        if stage + 1 >= STAGES[mode]:
            return
        if stage < 2 and (stage == 0) == (mode != "YR"):
            then = x_free = max(x_free, now) + (units / 2 if mode == "YR" else units)
            then += HOP
        else:
            share = 0.25 if stage == 2 else 0.5 if mode == "XR" else 1.0
            then = y_free = max(y_free, now) + units * share
            then += HOP
        ready[(b, stage + 1)] = then

    for b, (piece, first, width, _) in enumerate(BLOCKS):
        arrive = PIECE * (piece + (first + width) / BLOCK) - LEAD
        while ready:
            key = min(ready, key=ready.get)
            if ready[key] > now and ready[key] + ADDS > arrive:
                break
            run(*key)
        now = max(now, arrive) + MATMULS
        order.append(("block", b, 0))
        ready[(b, 0)] = now + SIB
    while ready:
        run(*min(ready, key=ready.get))
    return order


def moe_kernel(
    hid_hbm, ids_hbm, norm_hbm, router_hbm, gate_hbm, up_hbm, down_hbm, out,
    w_buf, hid, ids, norm_buf, router, normed, prob_buf, x_buf, act, g3, y_buf,
    part, sib_in, x_out, x_in, y_out, y_in, z_in, fin, fin_in,
    w_sem, load_sem, hid_send, hid_recv, ids_send, ids_recv,
    sib_send, sib_recv, xs_sem, xr_sem, ys_sem, yr_sem, zs_sem, zr_sem, fs_sem, fr_sem,
):
    me = lax.axis_index("ep")
    tp = lax.axis_index("tp")
    sib = me + 1 - 2 * (me % 2)
    across = (me + 2) % 4
    twin = 1 - tp
    sib_id, across_id, twin_id = {"ep": sib}, {"ep": across}, {"tp": twin}

    tok, dim = hid.shape[1], hid.shape[2]
    n_exp = router.shape[0]
    local_exp = act.shape[0]
    inner = act.shape[2]
    top_k = ids.shape[1]
    cap = x_buf.shape[1] // 4
    n_pieces = dim // BLOCK
    f32, bf16 = jnp.float32, jnp.bfloat16

    def gate_copies(pair):
        slot = pair % PAIR_SLOTS
        return [
            pltpu.make_async_copy(gate_hbm.at[pair], w_buf.at[slot, 0], w_sem.at[slot, 0]),
            pltpu.make_async_copy(up_hbm.at[pair], w_buf.at[slot, 1], w_sem.at[slot, 1]),
        ]

    def down_copy(piece, quad, first, width):
        slot = (local_exp + piece) % PAIR_SLOTS
        rows = 4 * inner
        return pltpu.make_async_copy(
            down_hbm.at[pl.ds(quad * rows, rows), pl.ds(piece * BLOCK + first, width)],
            w_buf.at[slot, quad // 2, :, pl.ds((quad % 2) * BLOCK + first, width)],
            w_sem.at[slot, quad + 4 * (first // LANES)],
        )

    def start_pair(pair):
        if pair < local_exp:
            for c in gate_copies(pair):
                c.start(priority=1)
        elif pair < local_exp + n_pieces:
            for piece, first, width, _ in BLOCKS:
                if piece == pair - local_exp:
                    for q in range(4):
                        down_copy(piece, q, first, width).start(priority=1)

    hid_load = pltpu.make_async_copy(hid_hbm, hid.at[0], load_sem.at[0])
    ids_load = pltpu.make_async_copy(ids_hbm, ids.at[0], load_sem.at[1])
    norm_load = pltpu.make_async_copy(norm_hbm, norm_buf, load_sem.at[2])
    router_load = pltpu.make_async_copy(router_hbm, router, load_sem.at[3])
    for c in (hid_load, ids_load, norm_load, router_load):
        c.start()
    for pair in range(PAIR_SLOTS):
        start_pair(pair)

    barrier = pltpu.get_barrier_semaphore()
    for dev in (sib_id, across_id, twin_id):
        pl.semaphore_signal(barrier, inc=1, device_id=dev, device_id_type=pl.DeviceIdType.MESH)
    pl.semaphore_wait(barrier, 3)

    def remote(src, dst, ssem, rsem, dev):
        return pltpu.make_async_remote_copy(
            src_ref=src, dst_ref=dst, send_sem=ssem, recv_sem=rsem,
            device_id=dev, device_id_type=pl.DeviceIdType.MESH,
        )

    def row_copies(j):
        src, dst, dev = ((0, 1, sib_id), (0, 2, across_id), (2, 3, sib_id))[j]
        return (
            remote(hid.at[src], hid.at[dst], hid_send.at[j], hid_recv.at[j], dev),
            remote(ids.at[src], ids.at[dst], ids_send.at[j], ids_recv.at[j], dev),
        )

    hid_load.wait()
    ids_load.wait()
    for j in (1, 0):
        for c in row_copies(j):
            c.start()
    norm_load.wait()
    router_load.wait()

    slot_iota = lax.broadcasted_iota(jnp.int32, (cap, tok), 0).astype(f32)
    exp_iota = lax.broadcasted_iota(jnp.int32, (local_exp, tok), 0) + me * local_exp
    t_row = lax.broadcasted_iota(jnp.int32, (tok, tok), 0)
    t_col = lax.broadcasted_iota(jnp.int32, (tok, tok), 1)
    before = jnp.where(t_row < t_col, 1.0, 0.0).astype(bf16)
    eye = jnp.where(t_row == t_col, 1.0, 0.0).astype(bf16)

    def prepare(k):
        acc = jnp.zeros((tok, LANES), f32)
        for i in range(dim // LANES):
            xs = hid[k, :, pl.ds(i * LANES, LANES)].astype(f32)
            acc = acc + xs * xs
        inv = lax.rsqrt(jnp.sum(acc, axis=1, keepdims=True) / dim + NORM_EPS)
        for i in range(dim // LANES):
            xs = hid[k, :, pl.ds(i * LANES, LANES)].astype(f32)
            w = norm_buf[pl.ds(i, 1), :].astype(f32)
            normed[:, pl.ds(i * LANES, LANES)] = (xs * inv * w).astype(bf16)
        logits = lax.dot_general(router[...], normed[...], (((1,), (1,)), ((), ())), preferred_element_type=f32)
        ex = jnp.exp(logits - jnp.max(logits, axis=0, keepdims=True))
        prob_buf[...] = ex / jnp.sum(ex, axis=0, keepdims=True)
        prob = prob_buf[pl.ds(pl.multiple_of(me * local_exp, local_exp), local_exp), :]
        hit = jnp.zeros((local_exp, tok), f32)
        for j in range(top_k):
            hit = hit + jnp.where(ids[k, pl.ds(j, 1), :] == exp_iota, 1.0, 0.0)
        rank = jnp.dot(hit.astype(bf16), before, preferred_element_type=f32)
        rank = jnp.where(hit > 0.5, rank, -1.0)
        place, weight = [], []
        for e in range(local_exp):
            here = rank[e : e + 1, :] == slot_iota
            place.append(jnp.where(here, 1.0, 0.0))
            weight.append(jnp.where(here, prob[e : e + 1, :], 0.0))
        place = jnp.concatenate(place, axis=0).astype(bf16)
        weight = jnp.concatenate(weight, axis=0)
        for p in range(3):
            piece = weight.astype(bf16)
            if p < 2:
                weight = weight - piece.astype(f32)
            g3[k, pl.ds(p * tok, tok), :] = lax.dot_general(
                eye, piece, (((1,), (1,)), ((), ())), preferred_element_type=f32
            ).astype(bf16)
        for c in range(dim // 512):
            rows = jnp.dot(place, normed[:, pl.ds(c * 512, 512)], preferred_element_type=f32).astype(bf16)
            x_buf[:, pl.ds(k * cap, cap), pl.ds(c * 512, 512)] = rows.reshape(local_exp, cap, 512)

    prepare(0)
    for c in row_copies(0):
        c.wait_recv()
    prepare(1)
    for c in row_copies(1):
        c.wait_recv()
    for c in row_copies(2):
        c.start()
    prepare(2)
    for c in row_copies(2):
        c.wait_recv()
    prepare(3)

    def twice(rows):
        return jnp.concatenate([rows, rows], axis=0)

    def experts(first, count):
        for i in range(count):
            for c in gate_copies(first + i):
                c.wait()
        for i in range(count):
            e = first + i
            slot = e % PAIR_SLOTS
            x = twice(x_buf[e])
            gate_pre = jnp.dot(x, w_buf[slot, 0], preferred_element_type=f32)[: 4 * cap]
            up_pre = jnp.dot(x, w_buf[slot, 1], preferred_element_type=f32)[: 4 * cap]
            act[e] = (jax.nn.silu(gate_pre) * up_pre).astype(bf16)

    more_pairs = (local_exp - PAIR_SLOTS) // 2

    def expert_step(i, carry):
        experts(2 * i, 2)
        for j in range(2):
            for c in gate_copies(2 * i + j + PAIR_SLOTS):
                c.start(priority=1)
        return carry

    lax.fori_loop(0, more_pairs, expert_step, 0)
    e = 2 * more_pairs
    while e < local_exp:
        count = 2 if e < local_exp - 2 else 1
        experts(e, count)
        for j in range(count):
            start_pair(e + j + PAIR_SLOTS)
        e += count

    def cols_of(b):
        piece, first, width, _ = BLOCKS[b]
        return piece * BLOCK + first, width

    def sib_copies(b):
        w = pl.ds(0, BLOCKS[b][2])
        return [
            remote(part.at[b, src, :, w], sib_in.at[b, i, :, w], sib_send.at[b, i], sib_recv.at[b, i], sib_id)
            for i, src in ((1, 3), (0, 1))
        ]

    def lanes(b, which):
        w = BLOCKS[b][2]
        if which == "all":
            return pl.ds(0, w)
        return pl.ds(pl.multiple_of((tp if which == "mine" else twin) * (w // 2), LANES), w // 2)

    def x_copy(b):
        w = lanes(b, "mine" if BLOCKS[b][3] == "YR" else "all")
        return remote(x_out.at[b, :, w], x_in.at[b, :, w], xs_sem.at[b], xr_sem.at[b], across_id)

    def y_copy(b):
        w = lanes(b, "theirs" if BLOCKS[b][3] in ("XR", "YR") else "all")
        return remote(y_out.at[b, :, w], y_in.at[b, :, w], ys_sem.at[b], yr_sem.at[b], twin_id)

    def z_copy(b):
        w = lanes(b, "theirs")
        return remote(x_out.at[b, :, w], z_in.at[b, :, w], zs_sem.at[b], zr_sem.at[b], twin_id)

    def fin_copy(b):
        return remote(fin.at[b], fin_in.at[b], fs_sem.at[b], fr_sem.at[b], twin_id)

    def compute(b):
        piece, first, width, _ = BLOCKS[b]
        slot = (local_exp + piece) % PAIR_SLOTS
        for q in range(4):
            down_copy(piece, q, first, width).wait()
        for q in range(4):
            for i in range(4):
                e = 4 * q + i
                w = w_buf[slot, q // 2, pl.ds(i * inner, inner), pl.ds((q % 2) * BLOCK + first, width)]
                y = jnp.dot(twice(act[e]), w, preferred_element_type=f32)[: 4 * cap].astype(bf16)
                for k in range(4):
                    y_buf[k, pl.ds(e * cap, cap), pl.ds(0, width)] = y[k * cap : (k + 1) * cap, :]
        for k in (3, 1, 2, 0):
            s = jnp.dot(g3[k], y_buf[k, :, pl.ds(0, width)], preferred_element_type=f32)
            part[b, k, :, pl.ds(0, width)] = s[:tok] + s[tok : 2 * tok] + s[2 * tok :]
            if k == 1:
                for c in sib_copies(b):
                    c.start()

    def put(b, which, value):
        start, width = cols_of(b)
        if which == "all":
            cols = pl.ds(start, width)
        else:
            half = width // 2
            cols = pl.ds(pl.multiple_of(start + (tp if which == "mine" else twin) * half, LANES), half)
        if which == "theirs":
            out[:, cols] = value
            return None
        result = (hid[0, :, cols].astype(f32) + value).astype(bf16)
        out[:, cols] = result
        return result

    def stage(b, n):
        mode = BLOCKS[b][3]
        full, mine = lanes(b, "all"), lanes(b, "mine") if mode in ("XR", "YR") else None
        if n == 0:
            first, second = sib_copies(b)
            first.wait_recv()
            x_out[b, :, full] = part[b, 2, :, full] + sib_in[b, 1, :, full]
            (z_copy if mode == "YR" else x_copy)(b).start()
            second.wait_recv()
            y_out[b, :, full] = part[b, 0, :, full] + sib_in[b, 0, :, full]
            if mode == "YR":
                y_copy(b).start()
        elif n == 1 and mode == "YR":
            z_copy(b).wait_recv()
            x_out[b, :, mine] = x_out[b, :, mine] + z_in[b, :, mine]
            x_copy(b).start()
            y_copy(b).wait_recv()
            y_out[b, :, mine] = y_out[b, :, mine] + y_in[b, :, mine]
        elif n == 1:
            x_copy(b).wait_recv()
            y_out[b, :, full] = y_out[b, :, full] + x_in[b, :, full]
            y_copy(b).start()
        elif mode == "X":
            y_copy(b).wait_recv()
            put(b, "all", y_out[b, :, full] + y_in[b, :, full])
        elif n == 2:
            (x_copy if mode == "YR" else y_copy)(b).wait_recv()
            other = x_in if mode == "YR" else y_in
            fin[b] = put(b, "mine", y_out[b, :, mine] + other[b, :, mine])
            fin_copy(b).start()
        else:
            fin_copy(b).wait_recv()
            put(b, "theirs", fin_in[b])

    for kind, b, n in static_order():
        if kind == "block":
            compute(b)
        else:
            stage(b, n)

    for j in range(3):
        for c in row_copies(j):
            c.wait_send()
    for b, (_, _, _, mode) in enumerate(BLOCKS):
        for c in sib_copies(b):
            c.wait_send()
        x_copy(b).wait_send()
        y_copy(b).wait_send()
        if mode == "YR":
            z_copy(b).wait_send()
        if mode in ("YR", "XR"):
            fin_copy(b).wait_send()


def solution(mesh):
    def per_device(hidden, expert_ids, norm_w, router_w, w_gate, w_up, w_down):
        tok, dim = hidden.shape
        top_k = expert_ids.shape[1]
        n_exp = router_w.shape[1]
        local_exp, _, inner = w_gate.shape
        cap = 8 * ((2 * top_k * tok + 8 * n_exp - 1) // (8 * n_exp))
        nb = len(BLOCKS)
        f32, bf16 = jnp.float32, jnp.bfloat16
        dma = pltpu.SemaphoreType.DMA
        hbm = pl.BlockSpec(memory_space=pl.ANY)
        return pl.pallas_call(
            moe_kernel,
            out_shape=pltpu.VMEM((tok, dim), bf16),
            in_specs=[hbm] * 7,
            out_specs=pl.BlockSpec(memory_space=pltpu.VMEM),
            scratch_shapes=[
                pltpu.VMEM((PAIR_SLOTS, 2, dim, inner), bf16),
                pltpu.VMEM((4, tok, dim), bf16),
                pltpu.VMEM((4, top_k, tok), jnp.int32),
                pltpu.VMEM((dim // LANES, LANES), bf16),
                pltpu.VMEM((n_exp, dim), bf16),
                pltpu.VMEM((tok, dim), bf16),
                pltpu.VMEM((n_exp, tok), f32),
                pltpu.VMEM((local_exp, 4 * cap, dim), bf16),
                pltpu.VMEM((local_exp, 4 * cap, inner), bf16),
                pltpu.VMEM((4, 3 * tok, local_exp * cap), bf16),
                pltpu.VMEM((4, local_exp * cap, BLOCK), bf16),
                pltpu.VMEM((nb, 4, tok, BLOCK), f32),
                pltpu.VMEM((nb, 2, tok, BLOCK), f32),
                pltpu.VMEM((nb, tok, BLOCK), f32),
                pltpu.VMEM((nb, tok, BLOCK), f32),
                pltpu.VMEM((nb, tok, BLOCK), f32),
                pltpu.VMEM((nb, tok, BLOCK), f32),
                pltpu.VMEM((nb, tok, BLOCK), f32),
                pltpu.VMEM((nb, tok, LANES), bf16),
                pltpu.VMEM((nb, tok, LANES), bf16),
                dma((PAIR_SLOTS, 8)),
                dma((4,)),
                dma((3,)), dma((3,)), dma((3,)), dma((3,)),
                dma((nb, 2)), dma((nb, 2)),
                *[dma((nb,))] * 8,
            ],
            compiler_params=pltpu.CompilerParams(
                collective_id=0, has_side_effects=True, vmem_limit_bytes=62 * 2**20,
            ),
            name="moe",
        )(
            hidden, expert_ids.T, norm_w.reshape(dim // LANES, LANES), router_w.T,
            w_gate, w_up, w_down.reshape(local_exp * inner, dim),
        )

    token_spec = P(("dp", "ep"), None)
    return jax.shard_map(
        per_device, mesh=mesh,
        in_specs=(token_spec, token_spec, P(None), P(None, None), P("ep", None, "tp"), P("ep", None, "tp"), P("ep", "tp", None)),
        out_specs=token_spec, check_vma=False,
    )
```
